32 devices in a mesh: part: 1 (over z), loc: 4 (over y), grp: 8 (over x, core).
Axes of the slice: x: 4, y: 4, z: 1, core: 2. Of those that a mesh axis runs over, the one named last changes fastest.
The devices are a block of a 4x4x8 slice.
Arguments:
- x_tok: bfloat16 [512, 2048], P(('part', 'grp', 'loc'))
- expert_ids: int32 [512, 6], P(('part', 'grp', 'loc'))
- gate_val: float32 [512, 6], P(('part', 'grp', 'loc'))
- w_gate: bfloat16 [64, 2048, 1408], P(('grp', 'loc'))
- w_up: bfloat16 [64, 2048, 1408], P(('grp', 'loc'))
- w_down: bfloat16 [64, 1408, 2048], P(('grp', 'loc'))
Outputs:
- output: bfloat16 [512, 2048], P(('part', 'grp', 'loc'))
All inputs are finite; a program needn't handle non-finite values.
Results may differ from the reference program's by a relative error of at most 0.0117678.
Values are sent between devices in bfloat16 or wider.
A program may use at most 768 MiB of HBM per device.

```python
import jax
import jax.numpy as jnp
from jax import lax

D = 2048
FF = 1408
EXPERTS = 64
TOP = 6
MAXG = 3
TOK_DEV = 16
GROUPS = 8
LOCS = 4

TOKENS = TOK_DEV * GROUPS * LOCS
PER_GROUP = EXPERTS // GROUPS
HIT_GROUPS = min(MAXG, GROUPS)
PER_HIT = TOP // HIT_GROUPS
CAP = 8 * (TOKENS * TOP // (4 * EXPERTS) + 1)
HOT_TOKENS = min(TOKENS, CAP * PER_GROUP // PER_HIT)


def draw_routing(route_key):
    key_grp, key_tok, key_exp = jax.random.split(route_key, 3)
    grp_order = jax.random.permutation(key_grp, GROUPS)
    tok_rank = jnp.arange(TOKENS)
    has_hot = tok_rank < HOT_TOKENS
    seq_base = jnp.where(has_hot, tok_rank * (HIT_GROUPS - 1), HOT_TOKENS * (HIT_GROUPS - 1) + (tok_rank - HOT_TOKENS) * HIT_GROUPS)
    choice = jnp.arange(HIT_GROUPS)
    other_pos = seq_base[:, None] + choice[None, :] - has_hot[:, None].astype(jnp.int32)
    other_grp = grp_order[1 + other_pos % (GROUPS - 1)]
    chosen = jnp.where(has_hot[:, None] & (choice[None, :] == 0), grp_order[0], other_grp)
    member = jnp.sum((chosen[:, :, None] == jnp.arange(GROUPS)[None, None, :]).astype(jnp.int32), axis=1)
    before = jnp.cumsum(member, axis=0) - member
    order_in = jnp.take_along_axis(before, chosen, axis=1)[:, :, None]
    pick_ids = jnp.arange(PER_HIT)[None, None, :]
    is_hot = (chosen == grp_order[0])[:, :, None]
    hot_seq = jnp.where(order_in < CAP, order_in * (PER_HIT - 1) + pick_ids - 1, CAP * (PER_HIT - 1) + (order_in - CAP) * PER_HIT + pick_ids)
    hot_slot = jnp.where((order_in < CAP) & (pick_ids == 0), 0, 1 + hot_seq % (PER_GROUP - 1))
    cold_slot = (order_in * PER_HIT + pick_ids) % PER_GROUP
    slot_pos = jnp.where(is_hot, hot_slot, cold_slot)
    grp_perm = jax.vmap(lambda sub_key: jax.random.permutation(sub_key, PER_GROUP))(jax.random.split(key_exp, GROUPS))
    local_ids = grp_perm[chosen[:, :, None], slot_pos]
    experts = (chosen[:, :, None] * PER_GROUP + local_ids).reshape(TOKENS, TOP)
    shuffle = jax.random.permutation(key_tok, TOKENS)
    return experts[shuffle].astype(jnp.int32)


def setup_inputs(seed: int = 0, part: int = 0) -> dict:
    root_key = jax.random.key(seed)
    key_part = jax.random.fold_in(root_key, part)
    key_x, key_route, key_gate = jax.random.split(key_part, 3)
    key_one, key_two, key_three = jax.random.split(jax.random.key(seed + 7919), 3)
    x_tok = jax.random.normal(key_x, (TOKENS, D), jnp.float32).astype(jnp.bfloat16)
    expert_ids = draw_routing(key_route)
    gate_val = jax.random.uniform(key_gate, (TOKENS, TOP), jnp.float32, 0.5, 1.5) * TOP ** -0.5
    w_gate = (jax.random.normal(key_one, (EXPERTS, D, FF), jnp.float32) * D ** -0.5).astype(jnp.bfloat16)
    w_up = (jax.random.normal(key_two, (EXPERTS, D, FF), jnp.float32) * D ** -0.5).astype(jnp.bfloat16)
    w_down = (jax.random.normal(key_three, (EXPERTS, FF, D), jnp.float32) * FF ** -0.5).astype(jnp.bfloat16)
    return {"x_tok": x_tok, "expert_ids": expert_ids, "gate_val": gate_val, "w_gate": w_gate, "w_up": w_up, "w_down": w_down}


def reference(x_tok, expert_ids, gate_val, w_gate, w_up, w_down):
    n_slots = TOKENS * TOP
    flat_ids = expert_ids.reshape(-1)
    sort_order = jnp.argsort(flat_ids, stable=True)
    sorted_ids = flat_ids[sort_order]
    counts = jnp.bincount(flat_ids, length=EXPERTS)
    starts = jnp.cumsum(counts) - counts
    slot_ids = sorted_ids * CAP + jnp.arange(n_slots) - starts[sorted_ids]
    src_tok = jnp.zeros(EXPERTS * CAP, jnp.int32).at[slot_ids].set((sort_order // TOP).astype(jnp.int32))
    src_gate = jnp.zeros(EXPERTS * CAP, jnp.float32).at[slot_ids].set(gate_val.reshape(-1)[sort_order])
    stacked = (src_tok.reshape(GROUPS, PER_GROUP, CAP), src_gate.reshape(GROUPS, PER_GROUP, CAP), w_gate.reshape(GROUPS, PER_GROUP, D, FF), w_up.reshape(GROUPS, PER_GROUP, D, FF), w_down.reshape(GROUPS, PER_GROUP, FF, D))

    def expert_step(group_acc, expert_in):
        tok_rows, row_gate, w_one, w_two, w_three = expert_in
        picked_rows = x_tok[tok_rows]
        up_gate = jnp.dot(picked_rows, w_one, preferred_element_type=jnp.float32)
        up_lin = jnp.dot(picked_rows, w_two, preferred_element_type=jnp.float32)
        hidden = (jax.nn.silu(up_gate) * up_lin).astype(jnp.bfloat16)
        out_rows = jnp.dot(hidden, w_three, preferred_element_type=jnp.float32)
        return group_acc.at[tok_rows].add(out_rows * row_gate[:, None]), None

    def group_step(y_acc, group_in):
        zero_acc = jnp.zeros((TOKENS, D), jnp.float32)
        group_sum = lax.scan(expert_step, zero_acc, group_in)[0]
        return y_acc + group_sum.astype(jnp.bfloat16).astype(jnp.float32), None

    y_sum = lax.scan(group_step, jnp.zeros((TOKENS, D), jnp.float32), stacked)[0]
    return y_sum.astype(jnp.bfloat16)
```

```python
import functools

import jax
import jax.numpy as jnp
from jax import lax
from jax.experimental import pallas as pl
from jax.experimental.pallas import tpu as pltpu
from jax.sharding import PartitionSpec as P

MESH = pl.DeviceIdType.MESH
F32, BF16 = jnp.float32, jnp.bfloat16
N_SUB = 2


def remote(src, dst, send_sem, recv_sem, device):
    return pltpu.make_async_remote_copy(src_ref=src, dst_ref=dst, send_sem=send_sem, recv_sem=recv_sem, device_id=device, device_id_type=MESH)


def layer_kernel(n_loc, n_grp, cap, top_k, x_ref, ids_ref, gate_ref, wg_hbm, wu_hbm, wd_hbm, out_ref,
                 wg, wu, wd, xall, mall, xg, hid, combine, ysend, yrecv, gpart, grecv, fin, frecv,
                 w_sem, m_send, m_recv, a_send, a_recv, b_send, b_recv, s_send, s_recv,
                 y_send, y_recv, g_send, g_recv, f_send, f_recv):
    n_x = n_grp // 2
    tok, d_model = x_ref.shape
    half = d_model // 2
    n_exp, _, d_ff = wg.shape
    per_group = n_exp * n_loc
    quarter = d_model // n_loc
    sub = quarter // N_SUB
    n_tok = n_grp * n_loc * tok
    slot_pad = yrecv.shape[2]

    l, g = lax.axis_index("loc"), lax.axis_index("grp")
    gx, gc = g // 2, g % 2

    def at_y(d):
        return (l + d + n_loc) % n_loc

    def at_x(d):
        return (gx + d + n_x) % n_x

    def at_g(d):
        return (g + d + n_grp) % n_grp

    def dev_y(d):
        return {"loc": at_y(d), "grp": g}

    def dev_x(d):
        return {"loc": l, "grp": at_x(d) * 2 + gc}

    def dev_g(d):
        return {"loc": l, "grp": at_g(d)}

    sibling = {"loc": l, "grp": gx * 2 + 1 - gc}

    loads = {}
    for e in range(n_exp):
        for j, (src, dst) in enumerate(((wg_hbm, wg), (wu_hbm, wu))):
            loads[e, j] = pltpu.make_async_copy(src.at[e], dst.at[e], w_sem.at[e, j])
            loads[e, j].start()
        for d in (2, 1, 3, 0):
            cols = pl.ds(pl.multiple_of(at_y(d) * quarter, quarter), quarter)
            loads[e, 2 + d] = pltpu.make_async_copy(wd_hbm.at[e, :, cols], wd.at[e, d], w_sem.at[e, 2 + d])
            loads[e, 2 + d].start()

    mall[gx, gc, l] = jnp.zeros(mall.shape[3:], F32)
    mall[gx, gc, l, :, 0:top_k] = ids_ref[...].astype(F32)
    mall[gx, gc, l, :, 8:8 + top_k] = gate_ref[...]
    xall[0, gx, gc, l] = x_ref[:, 0:half]
    xall[1, gx, gc, l] = x_ref[:, half:]

    barrier = pltpu.get_barrier_semaphore()
    for d in range(1, n_loc):
        pl.semaphore_signal(barrier, inc=1, device_id=dev_y(d), device_id_type=MESH)
    for d in range(1, n_grp):
        pl.semaphore_signal(barrier, inc=1, device_id=dev_g(d), device_id_type=MESH)
    pl.semaphore_wait(barrier, n_loc + n_grp - 2)

    sent = []

    def go(copy):
        copy.start()
        sent.append(copy)
        return copy

    m1 = [go(remote(mall.at[gx, gc, l], mall.at[gx, gc, l], m_send.at[d], m_recv.at[d], dev_y(d))) for d in range(1, n_loc)]
    a0 = [go(remote(x_ref.at[:, 0:half], xall.at[0, gx, gc, l], a_send.at[0, d], a_recv.at[0, d], dev_y(d))) for d in (2, 1, 3)]
    a1 = [go(remote(x_ref.at[:, half:d_model], xall.at[1, gx, gc, l], a_send.at[1, d], a_recv.at[1, d], dev_x(d))) for d in (2, 1, 3)]

    yrecv[:, :, cap:, :] = jnp.zeros((N_SUB, 2 * n_loc, slot_pad - cap, sub), F32)

    for c in m1:
        c.wait_recv()
    m2 = [go(remote(mall.at[gx, gc], mall.at[gx, gc], m_send.at[4 + d], m_recv.at[4 + d], dev_x(d))) for d in range(1, n_x)]
    ms = [go(remote(mall.at[gx, gc], mall.at[gx, gc], m_send.at[8], m_recv.at[8], sibling))]
    for c in a0:
        c.wait_recv()
    b0 = {d: go(remote(xall.at[0, gx, gc], xall.at[0, gx, gc], b_send.at[0, d], b_recv.at[0, d], dev_x(d))) for d in (2, 1, 3)}
    for c in a1:
        c.wait_recv()
    b1 = {d: go(remote(xall.at[1, :, gc, l], xall.at[1, :, gc, l], b_send.at[1, d], b_recv.at[1, d], dev_y(d))) for d in (2, 1, 3)}
    sib = [go(remote(xall.at[0, gx, gc], xall.at[0, gx, gc], s_send.at[0, 0], s_recv.at[0, 0], sibling))]
    sib.append(go(remote(xall.at[1, :, gc, l], xall.at[1, :, gc, l], s_send.at[1, 0], s_recv.at[1, 0], sibling)))
    for d in range(1, n_x):
        m2[d - 1].wait_recv()
        part = mall.at[at_x(-d), gc]
        ms.append(go(remote(part, part, m_send.at[8 + d], m_recv.at[8 + d], sibling)))
    for c in ms:
        c.wait_recv()

    meta = mall[...].reshape(n_tok, mall.shape[-1])
    lane = lax.broadcasted_iota(jnp.int32, meta.shape, 1)
    lane_exp = g * per_group + ((l + n_loc - lane // n_exp) % n_loc) * n_exp + lane % n_exp
    lane_exp = jnp.where(lane < per_group, lane_exp, -1).astype(F32)
    member = jnp.zeros(meta.shape, F32)
    gates = jnp.zeros(meta.shape, F32)
    for j in range(top_k):
        same = meta[:, j:j + 1] == lane_exp
        member = jnp.where(same, 1.0, member)
        gates = jnp.where(same, meta[:, 8 + j:9 + j], gates)
    tri_r = lax.broadcasted_iota(jnp.int32, (n_tok, n_tok), 0)
    tri_c = lax.broadcasted_iota(jnp.int32, (n_tok, n_tok), 1)
    before = jnp.dot(jnp.where(tri_c < tri_r, 1.0, 0.0).astype(BF16), member.astype(BF16), preferred_element_type=F32)
    slot = jnp.where(member > 0.0, before, -1.0)
    slot_lane = lax.broadcasted_iota(jnp.int32, (n_tok, slot_pad), 1).astype(F32)
    for b in range(per_group):
        combine[:, b * slot_pad:(b + 1) * slot_pad] = jnp.where(slot_lane == slot[:, b:b + 1], 1.0, 0.0).astype(BF16)
    slot_rows = jnp.transpose(slot)
    gate_rows = jnp.transpose(gates)
    cap_row = lax.broadcasted_iota(jnp.int32, (cap, n_tok), 0).astype(F32)
    picks, slot_gate = [], []
    for e in range(n_exp):
        hit = cap_row == slot_rows[e:e + 1, :]
        picks.append(jnp.where(hit, 1.0, 0.0).astype(BF16))
        slot_gate.append(jnp.sum(jnp.where(hit, gate_rows[e:e + 1, :], 0.0), axis=1, keepdims=True))

    for d in (1, 3, 2):
        b0[d].wait_recv()
        part = xall.at[0, at_x(-d), gc]
        sib.append(go(remote(part, part, s_send.at[0, d], s_recv.at[0, d], sibling)))
        b1[d].wait_recv()
        part = xall.at[1, :, gc, at_y(-d)]
        sib.append(go(remote(part, part, s_send.at[1, d], s_recv.at[1, d], sibling)))
    for c in sib:
        c.wait_recv()

    for e in range(n_exp):
        for h in range(2):
            rows = xall[h].reshape(n_tok, half)
            xg[e, :, h * half:(h + 1) * half] = jnp.dot(picks[e], rows, preferred_element_type=F32).astype(BF16)

    y_copies = {}
    for e in range(n_exp):
        loads[e, 0].wait()
        loads[e, 1].wait()
        rows = xg[e]
        tile = min(256, d_ff)
        for c0 in range(0, d_ff, tile):
            c1 = min(d_ff, c0 + tile)
            u = jnp.dot(rows, wg[e, :, c0:c1], preferred_element_type=F32)
            v = jnp.dot(rows, wu[e, :, c0:c1], preferred_element_type=F32)
            hid[e, :, c0:c1] = (jax.nn.silu(u) * v).astype(BF16)
        for d in (2, 1, 3):
            loads[e, 2 + d].wait()
            o = jnp.dot(hid[e], wd[e, d], preferred_element_type=F32) * slot_gate[e]
            for k in range(N_SUB):
                ysend[d - 1, e, k] = o[:, k * sub:(k + 1) * sub]
        for k in range(N_SUB):
            for d in (2, 1, 3):
                y_copies[e, k, d] = go(remote(ysend.at[d - 1, e, k], yrecv.at[k, n_exp * d + e, pl.ds(0, cap)], y_send.at[e, k, d], y_recv.at[e, k, d], dev_y(d)))
    for e in range(n_exp):
        loads[e, 2].wait()
        o = jnp.dot(hid[e], wd[e, 0], preferred_element_type=F32) * slot_gate[e]
        for k in range(N_SUB):
            yrecv[k, e, 0:cap, :] = o[:, k * sub:(k + 1) * sub]

    g_copies = {}
    for k in range(N_SUB):
        for e in range(n_exp):
            for d in (1, 3, 2):
                y_copies[e, k, d].wait_recv()
        vals = yrecv[k].reshape(per_group * slot_pad, sub)
        hi = vals.astype(BF16)
        rest = vals - hi.astype(F32)
        mid = rest.astype(BF16)
        low = (rest - mid.astype(F32)).astype(BF16)
        sel = combine[...]
        acc = jnp.dot(sel, hi, preferred_element_type=F32)
        acc += jnp.dot(sel, mid, preferred_element_type=F32)
        acc += jnp.dot(sel, low, preferred_element_type=F32)
        gpart[k] = acc.astype(BF16).reshape(n_grp, n_loc * tok, sub)
        for d in (4, 3, 5, 2, 6, 1, 7):
            g_copies[k, d] = go(remote(gpart.at[k, at_g(d)], grecv.at[k, d], g_send.at[k, d], g_recv.at[k, d], dev_g(d)))

    f_copies = {}
    for k in range(N_SUB):
        total = gpart[k, g].astype(F32)
        for d in range(1, n_grp):
            g_copies[k, d].wait_recv()
            total += grecv[k, d].astype(F32)
        fin[k] = total.astype(BF16).reshape(n_loc, tok, sub)
        for d in (2, 1, 3):
            f_copies[k, d] = go(remote(fin.at[k, at_y(d)], frecv.at[k, d], f_send.at[k, d], f_recv.at[k, d], dev_y(d)))
    for k in range(N_SUB):
        for d in range(n_loc):
            if d:
                f_copies[k, d].wait_recv()
            cols = pl.ds(pl.multiple_of(at_y(-d) * quarter + k * sub, sub), sub)
            out_ref[:, cols] = frecv[k, d] if d else fin[k, l]
    for c in sent:
        c.wait_send()


def solution(mesh):
    n_grp, n_loc = mesh.shape["grp"], mesh.shape["loc"]
    tok_spec = P(("part", "grp", "loc"), None)
    w_spec = P(("grp", "loc"), None, None)

    def device_step(x_tok, expert_ids, gate_val, w_gate, w_up, w_down):
        tok, d_model = x_tok.shape
        top_k = expert_ids.shape[1]
        n_exp, _, d_ff = w_gate.shape
        n_tok = tok * n_grp * n_loc
        cap = 8 * (n_tok * top_k // (4 * n_exp * n_loc * n_grp) + 1)
        slot_pad = -(-cap // 128) * 128
        quarter = d_model // n_loc
        sub = quarter // N_SUB
        dma = pltpu.SemaphoreType.DMA
        vmem = pl.BlockSpec(memory_space=pltpu.VMEM)
        hbm = pl.BlockSpec(memory_space=pl.ANY)
        return pl.pallas_call(
            functools.partial(layer_kernel, n_loc, n_grp, cap, top_k),
            out_shape=jax.ShapeDtypeStruct((tok, d_model), BF16),
            in_specs=[vmem, vmem, vmem, hbm, hbm, hbm],
            out_specs=vmem,
            scratch_shapes=[
                pltpu.VMEM((n_exp, d_model, d_ff), BF16),
                pltpu.VMEM((n_exp, d_model, d_ff), BF16),
                pltpu.VMEM((n_exp, n_loc, d_ff, quarter), BF16),
                pltpu.VMEM((2, n_grp // 2, 2, n_loc, tok, d_model // 2), BF16),
                pltpu.VMEM((n_grp // 2, 2, n_loc, tok, 128), F32),
                pltpu.VMEM((n_exp, cap, d_model), BF16),
                pltpu.VMEM((n_exp, cap, d_ff), BF16),
                pltpu.VMEM((n_tok, n_exp * n_loc * slot_pad), BF16),
                pltpu.VMEM((n_loc - 1, n_exp, N_SUB, cap, sub), F32),
                pltpu.VMEM((N_SUB, n_exp * n_loc, slot_pad, sub), F32),
                pltpu.VMEM((N_SUB, n_grp, n_loc * tok, sub), BF16),
                pltpu.VMEM((N_SUB, n_grp, n_loc * tok, sub), BF16),
                pltpu.VMEM((N_SUB, n_loc, tok, sub), BF16),
                pltpu.VMEM((N_SUB, n_loc, tok, sub), BF16),
                dma((n_exp, 2 + n_loc)),
                dma((12,)), dma((12,)),
                dma((2, 4)), dma((2, 4)),
                dma((2, 4)), dma((2, 4)),
                dma((2, 4)), dma((2, 4)),
                dma((n_exp, N_SUB, n_loc)), dma((n_exp, N_SUB, n_loc)),
                dma((N_SUB, n_grp)), dma((N_SUB, n_grp)),
                dma((N_SUB, n_loc)), dma((N_SUB, n_loc)),
            ],
            compiler_params=pltpu.CompilerParams(collective_id=0, has_side_effects=True, vmem_limit_bytes=64000 * 1024),
        )(x_tok, expert_ids, gate_val, w_gate, w_up, w_down)

    return jax.shard_map(device_step, mesh=mesh, in_specs=(tok_spec, tok_spec, tok_spec, w_spec, w_spec, w_spec), out_specs=tok_spec, check_vma=False)
```

```python
import functools

import jax
import jax.numpy as jnp
from jax import lax
from jax.experimental import pallas as pl
from jax.experimental.pallas import tpu as pltpu
from jax.sharding import PartitionSpec as P

MESH = pl.DeviceIdType.MESH
F32, BF16 = jnp.float32, jnp.bfloat16
N_SUB = 4
N_CHUNK = 4


def remote(src, dst, send_sem, recv_sem, device):
    return pltpu.make_async_remote_copy(src_ref=src, dst_ref=dst, send_sem=send_sem, recv_sem=recv_sem, device_id=device, device_id_type=MESH)


def layer_kernel(n_loc, n_grp, cap, top_k, x_ref, ids_ref, gate_ref, wg_hbm, wu_hbm, wd_hbm, out_ref,
                 wg, wu, wd, xall, mown, mcol, mrow, mall, tri, picks, xg, uacc, vacc, hid, combine, ysend, yrecv, gpart, grecv, fin, frecv,
                 w_sem, m_send, m_recv, r_send, r_recv, a_send, a_recv, b_send, b_recv, s_send, s_recv,
                 y_send, y_recv, g_send, g_recv, f_send, f_recv):
    n_x = n_grp // 2
    tok, d_model = x_ref.shape
    width = d_model // N_CHUNK
    n_exp, _, d_ff = wg.shape
    per_group = n_exp * n_loc
    quarter = d_model // n_loc
    sub = quarter // N_SUB
    n_tok = n_grp * n_loc * tok
    slot_pad = yrecv.shape[2]
    cap_pad = hid.shape[1]

    l, g = lax.axis_index("loc"), lax.axis_index("grp")
    gx, gc = g // 2, g % 2

    def at_y(d):
        return (l + d + n_loc) % n_loc

    def at_x(d):
        return (gx + d + n_x) % n_x

    def at_g(d):
        return (g + d + n_grp) % n_grp

    def dev_y(d):
        return {"loc": at_y(d), "grp": g}

    def dev_x(d):
        return {"loc": l, "grp": at_x(d) * 2 + gc}

    def dev_g(d):
        return {"loc": l, "grp": at_g(d)}

    sibling = {"loc": l, "grp": gx * 2 + 1 - gc}

    barrier = pltpu.get_barrier_semaphore()
    for d in range(1, n_loc):
        pl.semaphore_signal(barrier, inc=1, device_id=dev_y(d), device_id_type=MESH)
    for d in range(1, n_grp):
        pl.semaphore_signal(barrier, inc=1, device_id=dev_g(d), device_id_type=MESH)

    loads = {}
    for e in range(n_exp):
        for j, (src, dst) in enumerate(((wg_hbm, wg), (wu_hbm, wu))):
            loads[e, j] = pltpu.make_async_copy(src.at[e], dst.at[e], w_sem.at[e, j])
            loads[e, j].start()
    for e in range(n_exp):
        for d in (2, 1, 3, 0):
            cols = pl.ds(pl.multiple_of(at_y(d) * quarter, quarter), quarter)
            loads[e, 2 + d] = pltpu.make_async_copy(wd_hbm.at[e, :, cols], wd.at[e, d], w_sem.at[e, 2 + d])
            loads[e, 2 + d].start()

    mown[...] = jnp.zeros(mown.shape, F32)
    mown[0:top_k, 0:tok] = ids_ref[...].astype(F32)
    mown[8:8 + top_k, 0:tok] = gate_ref[...]
    mown[...] = pltpu.roll(mown[...], gc * (n_loc * tok) + l * tok, 1)
    for h in range(N_CHUNK):
        xall[h, gx, gc, l] = x_ref[:, h * width:(h + 1) * width]
    tri_r = lax.broadcasted_iota(jnp.int32, (n_tok, n_tok), 0)
    tri_c = lax.broadcasted_iota(jnp.int32, (n_tok, n_tok), 1)
    tri[...] = jnp.where(tri_r < tri_c, 1.0, 0.0).astype(BF16)
    yrecv[:, :, cap:, :] = jnp.zeros((N_SUB, per_group, slot_pad - cap, sub), F32)

    pl.semaphore_wait(barrier, n_loc + n_grp - 2)

    sent = []

    def go(copy):
        copy.start()
        sent.append(copy)
        return copy

    far_first, near_first = (2, 1, 3), (1, 3, 2)
    m1 = [go(remote(mown, mcol.at[d], m_send.at[d], m_recv.at[d], dev_y(d))) for d in far_first]
    a = {}
    for h in range(N_CHUNK):
        for d in far_first:
            a[h, d] = go(remote(x_ref.at[:, h * width:(h + 1) * width], xall.at[h, gx, gc, l], a_send.at[h, d], a_recv.at[h, d], dev_x(d) if h % 2 else dev_y(d)))
    for c in m1:
        c.wait_recv()
    mrow[...] = mown[...] + mcol[1] + mcol[2] + mcol[3]
    mall[g] = mrow[...]
    m2 = [go(remote(mrow, mall.at[g], r_send.at[d], r_recv.at[d], dev_g(d))) for d in range(1, n_grp)]

    def region(h, d):
        return xall.at[h, :, gc, at_y(-d)] if h % 2 else xall.at[h, at_x(-d), gc]

    b, sib = {}, {}

    def relay(h, d):
        sib[h, d] = go(remote(region(h, d), region(h, d), s_send.at[h, d], s_recv.at[h, d], sibling))

    for h in range(N_CHUNK):
        for d in near_first:
            a[h, d].wait_recv()
        for d in far_first:
            b[h, d] = go(remote(region(h, 0), region(h, 0), b_send.at[h, d], b_recv.at[h, d], dev_y(d) if h % 2 else dev_x(d)))
        relay(h, 0)

    for c in m2:
        c.wait_recv()
    meta = jnp.concatenate([mall[2 * i] + mall[2 * i + 1] for i in range(n_x)], axis=1)
    row = lax.broadcasted_iota(jnp.int32, (per_group, n_tok), 0)
    row_exp = (g * per_group + ((l + n_loc - row // n_exp) % n_loc) * n_exp + row % n_exp).astype(F32)
    member = jnp.zeros(row.shape, F32)
    gates = jnp.zeros(row.shape, F32)
    for j in range(top_k):
        same = meta[j:j + 1, :] == row_exp
        member = jnp.where(same, 1.0, member)
        gates = jnp.where(same, meta[8 + j:9 + j, :], gates)
    before = jnp.dot(member.astype(BF16), tri[...], preferred_element_type=F32)
    slot = jnp.where(member > 0.0, before, -1.0)
    cap_row = lax.broadcasted_iota(jnp.int32, (cap_pad, n_tok), 0).astype(F32)
    slot_gate = []
    for e in range(n_exp):
        hit = cap_row == slot[e:e + 1, :]
        picks[e * cap_pad:(e + 1) * cap_pad, :] = jnp.where(hit, 1.0, 0.0).astype(BF16)
        slot_gate.append(jnp.sum(jnp.where(hit, gates[e:e + 1, :], 0.0), axis=1, keepdims=True))

    tile = min(256, d_ff)
    tiles = [(c0, min(d_ff, c0 + tile)) for c0 in range(0, d_ff, tile)]
    for p in range(N_CHUNK // 2):
        pair = (2 * p, 2 * p + 1)
        for d in near_first:
            for h in pair:
                b[h, d].wait_recv()
                relay(h, d)
        for h in pair:
            for d in (0,) + near_first:
                sib[h, d].wait_recv()
        for h in pair:
            rows = xall[h].reshape(n_tok, width)
            got = jnp.dot(picks[...], rows, preferred_element_type=F32).astype(BF16)
            for e in range(n_exp):
                xg[e, :, h * width:(h + 1) * width] = got[e * cap_pad:(e + 1) * cap_pad]
        k0, k1 = 2 * p * width, 2 * (p + 1) * width
        if p == 0:
            for e in range(n_exp):
                loads[e, 0].wait()
                loads[e, 1].wait()
                for c0, c1 in tiles:
                    uacc[e, :, c0:c1] = jnp.dot(xg[e, :, k0:k1], wg[e, k0:k1, c0:c1], preferred_element_type=F32)
                    vacc[e, :, c0:c1] = jnp.dot(xg[e, :, k0:k1], wu[e, k0:k1, c0:c1], preferred_element_type=F32)
    y_copies = {}
    for e in range(n_exp):
        for c0, c1 in tiles:
            u = uacc[e, :, c0:c1] + jnp.dot(xg[e, :, k0:k1], wg[e, k0:k1, c0:c1], preferred_element_type=F32)
            v = vacc[e, :, c0:c1] + jnp.dot(xg[e, :, k0:k1], wu[e, k0:k1, c0:c1], preferred_element_type=F32)
            hid[e, :, c0:c1] = (jax.nn.silu(u) * v).astype(BF16)

        def send_rows(e, k, d):
            y_copies[e, k, d] = go(remote(ysend.at[d - 1, e, k, pl.ds(0, cap)], yrecv.at[k, n_exp * d + e, pl.ds(0, cap)], y_send.at[e, k, d], y_recv.at[e, k, d], dev_y(d)))

        for d in far_first:
            loads[e, 2 + d].wait()
            o = jnp.dot(hid[e], wd[e, d], preferred_element_type=F32) * slot_gate[e]
            for k in range(N_SUB):
                ysend[d - 1, e, k] = o[:, k * sub:(k + 1) * sub]
            if e + 1 < n_exp:
                for k in range(N_SUB):
                    send_rows(e, k, d)
        if e + 1 == n_exp:
            for k in range(N_SUB):
                for d in far_first:
                    send_rows(e, k, d)
    for e in range(n_exp):
        loads[e, 2].wait()
        o = jnp.dot(hid[e], wd[e, 0], preferred_element_type=F32) * slot_gate[e]
        for k in range(N_SUB):
            yrecv[k, e, 0:cap, :] = o[0:cap, k * sub:(k + 1) * sub]
    slot_cols = jnp.transpose(jnp.concatenate([slot, jnp.zeros((128 - per_group, n_tok), F32)], axis=0))
    slot_lane = lax.broadcasted_iota(jnp.int32, (n_tok, slot_pad), 1).astype(F32)
    for i in range(per_group):
        combine[:, i * slot_pad:(i + 1) * slot_pad] = jnp.where(slot_lane == slot_cols[:, i:i + 1], 1.0, 0.0).astype(BF16)

    g_copies = {}
    for k in range(N_SUB):
        for e in range(n_exp):
            for d in near_first:
                y_copies[e, k, d].wait_recv()
        vals = yrecv[k].reshape(per_group * slot_pad, sub)
        hi = vals.astype(BF16)
        rest = vals - hi.astype(F32)
        mid = rest.astype(BF16)
        low = (rest - mid.astype(F32)).astype(BF16)
        sel = combine[...]
        acc = jnp.dot(sel, hi, preferred_element_type=F32)
        acc += jnp.dot(sel, mid, preferred_element_type=F32)
        acc += jnp.dot(sel, low, preferred_element_type=F32)
        gpart[k] = acc.astype(BF16).reshape(n_grp, n_loc * tok, sub)
        for d in (4, 3, 5, 2, 6, 1, 7):
            g_copies[k, d] = go(remote(gpart.at[k, at_g(d)], grecv.at[k, d], g_send.at[k, d], g_recv.at[k, d], dev_g(d)))

    f_copies = {}
    for k in range(N_SUB):
        total = gpart[k, g].astype(F32)
        for d in range(1, n_grp):
            g_copies[k, d].wait_recv()
            total += grecv[k, d].astype(F32)
        fin[k] = total.astype(BF16).reshape(n_loc, tok, sub)
        for d in far_first:
            f_copies[k, d] = go(remote(fin.at[k, at_y(d)], frecv.at[k, d], f_send.at[k, d], f_recv.at[k, d], dev_y(d)))
    for k in range(N_SUB):
        for d in range(n_loc):
            if d:
                f_copies[k, d].wait_recv()
            cols = pl.ds(pl.multiple_of(at_y(-d) * quarter + k * sub, sub), sub)
            out_ref[:, cols] = frecv[k, d] if d else fin[k, l]
    for c in sent:
        c.wait_send()


def solution(mesh):
    n_grp, n_loc = mesh.shape["grp"], mesh.shape["loc"]
    tok_spec = P(("part", "grp", "loc"), None)
    w_spec = P(("grp", "loc"), None, None)

    def device_step(x_tok, expert_ids, gate_val, w_gate, w_up, w_down):
        tok, d_model = x_tok.shape
        top_k = expert_ids.shape[1]
        n_exp, _, d_ff = w_gate.shape
        n_tok = tok * n_grp * n_loc
        per_group = n_exp * n_loc
        cap = 8 * (n_tok * top_k // (4 * per_group * n_grp) + 1)
        slot_pad = -(-cap // 128) * 128
        cap_pad = -(-cap // 16) * 16
        quarter = d_model // n_loc
        sub = quarter // N_SUB
        dma = pltpu.SemaphoreType.DMA
        vmem = pl.BlockSpec(memory_space=pltpu.VMEM)
        hbm = pl.BlockSpec(memory_space=pl.ANY)
        return pl.pallas_call(
            functools.partial(layer_kernel, n_loc, n_grp, cap, top_k),
            out_shape=jax.ShapeDtypeStruct((tok, d_model), BF16),
            in_specs=[vmem, vmem, vmem, hbm, hbm, hbm],
            out_specs=vmem,
            scratch_shapes=[
                pltpu.VMEM((n_exp, d_model, d_ff), BF16),
                pltpu.VMEM((n_exp, d_model, d_ff), BF16),
                pltpu.VMEM((n_exp, n_loc, d_ff, quarter), BF16),
                pltpu.VMEM((N_CHUNK, n_grp // 2, 2, n_loc, tok, d_model // N_CHUNK), BF16),
                pltpu.VMEM((16, 128), F32),
                pltpu.VMEM((n_loc, 16, 128), F32),
                pltpu.VMEM((16, 128), F32),
                pltpu.VMEM((n_grp, 16, 128), F32),
                pltpu.VMEM((n_tok, n_tok), BF16),
                pltpu.VMEM((n_exp * cap_pad, n_tok), BF16),
                pltpu.VMEM((n_exp, cap_pad, d_model), BF16),
                pltpu.VMEM((n_exp, cap_pad, d_ff), F32),
                pltpu.VMEM((n_exp, cap_pad, d_ff), F32),
                pltpu.VMEM((n_exp, cap_pad, d_ff), BF16),
                pltpu.VMEM((n_tok, per_group * slot_pad), BF16),
                pltpu.VMEM((n_loc - 1, n_exp, N_SUB, cap_pad, sub), F32),
                pltpu.VMEM((N_SUB, per_group, slot_pad, sub), F32),
                pltpu.VMEM((N_SUB, n_grp, n_loc * tok, sub), BF16),
                pltpu.VMEM((N_SUB, n_grp, n_loc * tok, sub), BF16),
                pltpu.VMEM((N_SUB, n_loc, tok, sub), BF16),
                pltpu.VMEM((N_SUB, n_loc, tok, sub), BF16),
                dma((n_exp, 2 + n_loc)),
                dma((n_loc,)), dma((n_loc,)),
                dma((n_grp,)), dma((n_grp,)),
                dma((N_CHUNK, 4)), dma((N_CHUNK, 4)),
                dma((N_CHUNK, 4)), dma((N_CHUNK, 4)),
                dma((N_CHUNK, 4)), dma((N_CHUNK, 4)),
                dma((n_exp, N_SUB, n_loc)), dma((n_exp, N_SUB, n_loc)),
                dma((N_SUB, n_grp)), dma((N_SUB, n_grp)),
                dma((N_SUB, n_loc)), dma((N_SUB, n_loc)),
            ],
            compiler_params=pltpu.CompilerParams(collective_id=0, has_side_effects=True, vmem_limit_bytes=64000 * 1024),
        )(x_tok, expert_ids.T, gate_val.T, w_gate, w_up, w_down)

    return jax.shard_map(device_step, mesh=mesh, in_specs=(tok_spec, tok_spec, tok_spec, w_spec, w_spec, w_spec), out_specs=tok_spec, check_vma=False)
```

```python
import functools

import jax
import jax.numpy as jnp
from jax import lax
from jax.experimental import pallas as pl
from jax.experimental.pallas import tpu as pltpu
from jax.sharding import PartitionSpec as P

MESH = pl.DeviceIdType.MESH
F32, BF16 = jnp.float32, jnp.bfloat16
N_SUB = 4
N_CHUNK = 4


def remote(src, dst, send_sem, recv_sem, device):
    return pltpu.make_async_remote_copy(src_ref=src, dst_ref=dst, send_sem=send_sem, recv_sem=recv_sem, device_id=device, device_id_type=MESH)


def drain(ref, sem):
    pltpu.make_async_copy(ref, ref, sem).wait()


def layer_kernel(n_loc, n_grp, cap, top_k, x_ref, ids_ref, gate_ref, wg_hbm, wu_hbm, wd_hbm, out_ref,
                 wg, wu, wd, xall, mown, mcol, mrow, mall, tri, picks, xg, uacc, vacc, hid, combine, ysend, yrecv, gpart, grecv, fin, frecv,
                 w_sem, m_send, m_recv, a_send, a_recv, b_send, b_recv, s_send, s_recv,
                 y_send, y_recv, g_send, g_recv, f_send, f_recv):
    n_x = n_grp // 2
    tok, d_model = x_ref.shape
    width = d_model // N_CHUNK
    n_exp, _, d_ff = wg.shape
    per_group = n_exp * n_loc
    quarter = d_model // n_loc
    sub = quarter // N_SUB
    n_tok = n_grp * n_loc * tok
    slot_pad = yrecv.shape[2]
    cap_pad = hid.shape[1]

    l, g = lax.axis_index("loc"), lax.axis_index("grp")
    gx, gc = g // 2, g % 2

    def at_y(d):
        return (l + d + n_loc) % n_loc

    def at_x(d):
        return (gx + d + n_x) % n_x

    def at_g(d):
        return (g + d + n_grp) % n_grp

    def dev_y(d):
        return {"loc": at_y(d), "grp": g}

    def dev_x(d):
        return {"loc": l, "grp": at_x(d) * 2 + gc}

    def dev_g(d):
        return {"loc": l, "grp": at_g(d)}

    sibling = {"loc": l, "grp": gx * 2 + 1 - gc}

    barrier = pltpu.get_barrier_semaphore()
    for d in range(1, n_loc):
        pl.semaphore_signal(barrier, inc=1, device_id=dev_y(d), device_id_type=MESH)
    for d in range(1, n_grp):
        pl.semaphore_signal(barrier, inc=1, device_id=dev_g(d), device_id_type=MESH)

    loads = {}
    for e in range(n_exp):
        for j, (src, dst) in enumerate(((wg_hbm, wg), (wu_hbm, wu))):
            loads[e, j] = pltpu.make_async_copy(src.at[e], dst.at[e], w_sem.at[e, j])
            loads[e, j].start()
    for e in range(n_exp):
        for d in (2, 1, 3, 0):
            cols = pl.ds(pl.multiple_of(at_y(d) * quarter, quarter), quarter)
            loads[e, 2 + d] = pltpu.make_async_copy(wd_hbm.at[e, :, cols], wd.at[e, d], w_sem.at[e, 2])
            loads[e, 2 + d].start()

    lanes = n_loc * tok
    mown[...] = jnp.zeros(mown.shape, F32)
    mown[0:top_k, 0:tok] = ids_ref[...].astype(F32)
    mown[0:top_k, lanes:lanes + tok] = gate_ref[...]
    mown[...] = pltpu.roll(mown[...], l * tok, 1)
    xall[gx, gc, l] = x_ref[...]
    tri_r = lax.broadcasted_iota(jnp.int32, (n_tok, n_tok), 0)
    tri_c = lax.broadcasted_iota(jnp.int32, (n_tok, n_tok), 1)
    tri[...] = jnp.where(tri_r < tri_c, 1.0, 0.0).astype(BF16)
    yrecv[:, :, cap:, :] = jnp.zeros((N_SUB, per_group, slot_pad - cap, sub), F32)

    pl.semaphore_wait(barrier, n_loc + n_grp - 2)

    def go(copy):
        copy.start()

    far_first, near_first = (2, 1, 3), (1, 3, 2)
    for d in far_first:
        go(remote(mown, mcol.at[d], m_send, m_recv.at[0], dev_y(d)))

    def half(p):
        return pl.ds(p * 2 * width, 2 * width)

    for p in range(2):
        for d in far_first:
            for axis in range(2):
                go(remote(x_ref.at[:, half(p)], xall.at[gx, gc, l, :, half(p)], a_send, a_recv.at[axis, p, d - 1], dev_x(d) if axis else dev_y(d)))
    drain(mcol.at[pl.ds(1, n_loc - 1)], m_recv.at[0])
    mrow[...] = mown[...] + mcol[1] + mcol[2] + mcol[3]
    mall[gx, gc] = mrow[...]
    for d in far_first:
        go(remote(mrow, mall.at[gx, gc], m_send, m_recv.at[1], dev_x(d)))
    go(remote(mrow, mall.at[gx, gc], m_send, m_recv.at[2], sibling))

    def relay(p, d):
        part = xall.at[at_x(-d), gc, :, :, half(p)]
        go(remote(part, part, s_send, s_recv.at[p], sibling))

    for p in range(2):
        for d in near_first:
            for axis in range(2):
                drain(xall.at[at_x(-d), gc, l, :, half(p)] if axis else xall.at[gx, gc, at_y(-d), :, half(p)], a_recv.at[axis, p, d - 1])
                cols = pl.ds((2 * p + axis) * width, width)
                part = xall.at[at_x(-d), gc, l, :, cols] if axis else xall.at[gx, gc, at_y(-d), :, cols]
                for t in far_first:
                    go(remote(part, part, b_send, b_recv.at[p, (d if axis else t) - 1], dev_y(t) if axis else dev_x(t)))
        relay(p, 0)
        if p == 0:
            drain(mall.at[pl.ds(0, n_x - 1), 0], m_recv.at[1])
            for d in near_first:
                part = mall.at[at_x(-d), gc]
                go(remote(part, part, m_send, m_recv.at[2], sibling))

    drain(mall.at[:, 0], m_recv.at[2])
    lane = lax.broadcasted_iota(jnp.int32, mall.shape[2:], 1)
    ids = jnp.concatenate([jnp.where(lane < lanes, mall[i, 0], pltpu.roll(mall[i, 1], lanes, 1)) for i in range(n_x)], axis=1)
    gate_of = jnp.concatenate([jnp.where(lane < lanes, pltpu.roll(mall[i, 0], lanes, 1), mall[i, 1]) for i in range(n_x)], axis=1)
    row = lax.broadcasted_iota(jnp.int32, (per_group, n_tok), 0)
    row_exp = (g * per_group + ((l + n_loc - row // n_exp) % n_loc) * n_exp + row % n_exp).astype(F32)
    member = jnp.zeros(row.shape, F32)
    gates = jnp.zeros(row.shape, F32)
    for j in range(top_k):
        same = ids[j:j + 1, :] == row_exp
        member = jnp.where(same, 1.0, member)
        gates = jnp.where(same, gate_of[j:j + 1, :], gates)
    before = jnp.dot(member.astype(BF16), tri[...], preferred_element_type=F32)
    slot = jnp.where(member > 0.0, before, -1.0)
    cap_row = lax.broadcasted_iota(jnp.int32, (cap_pad, n_tok), 0).astype(F32)
    slot_gate = []
    for e in range(n_exp):
        hit = cap_row == slot[e:e + 1, :]
        picks[e * cap_pad:(e + 1) * cap_pad, :] = jnp.where(hit, 1.0, 0.0).astype(BF16)
        slot_gate.append(jnp.sum(jnp.where(hit, gates[e:e + 1, :], 0.0), axis=1, keepdims=True))

    tile = min(256, d_ff)
    tiles = [(c0, min(d_ff, c0 + tile)) for c0 in range(0, d_ff, tile)]
    for p in range(2):
        for d in near_first:
            drain(xall.at[at_x(-d), gc, pl.ds(0, n_loc - 1), :, half(p)], b_recv.at[p, d - 1])
            relay(p, d)
        drain(xall.at[:, 1 - gc, :, :, half(p)], s_recv.at[p])
        for h in (2 * p, 2 * p + 1):
            rows = xall[:, :, :, :, h * width:(h + 1) * width].reshape(n_tok, width)
            got = jnp.dot(picks[...], rows, preferred_element_type=F32).astype(BF16)
            for e in range(n_exp):
                xg[e, :, h * width:(h + 1) * width] = got[e * cap_pad:(e + 1) * cap_pad]
        k0, k1 = 2 * p * width, 2 * (p + 1) * width
        if p == 0:
            for e in range(n_exp):
                loads[e, 0].wait()
                loads[e, 1].wait()
                for c0, c1 in tiles:
                    uacc[e, :, c0:c1] = jnp.dot(xg[e, :, k0:k1], wg[e, k0:k1, c0:c1], preferred_element_type=F32)
                    vacc[e, :, c0:c1] = jnp.dot(xg[e, :, k0:k1], wu[e, k0:k1, c0:c1], preferred_element_type=F32)
    for e in range(n_exp):
        for c0, c1 in tiles:
            u = uacc[e, :, c0:c1] + jnp.dot(xg[e, :, k0:k1], wg[e, k0:k1, c0:c1], preferred_element_type=F32)
            v = vacc[e, :, c0:c1] + jnp.dot(xg[e, :, k0:k1], wu[e, k0:k1, c0:c1], preferred_element_type=F32)
            hid[e, :, c0:c1] = (jax.nn.silu(u) * v).astype(BF16)

        def send_rows(e, k, d):
            go(remote(ysend.at[d - 1, e, k, pl.ds(0, cap)], yrecv.at[k, n_exp * d + e, pl.ds(0, cap)], y_send, y_recv.at[k], dev_y(d)))

        drain(wd.at[e], w_sem.at[e, 2])
        for d in far_first:
            o = jnp.dot(hid[e], wd[e, d], preferred_element_type=F32) * slot_gate[e]
            for k in range(N_SUB):
                ysend[d - 1, e, k] = o[:, k * sub:(k + 1) * sub]
            if e + 1 < n_exp:
                for k in range(N_SUB):
                    send_rows(e, k, d)
        if e + 1 == n_exp:
            for k in range(N_SUB):
                for d in far_first:
                    send_rows(e, k, d)
    for e in range(n_exp):
        o = jnp.dot(hid[e], wd[e, 0], preferred_element_type=F32) * slot_gate[e]
        for k in range(N_SUB):
            yrecv[k, e, 0:cap, :] = o[0:cap, k * sub:(k + 1) * sub]
    slot_cols = jnp.transpose(jnp.concatenate([slot, jnp.zeros((128 - per_group, n_tok), F32)], axis=0))
    slot_lane = lax.broadcasted_iota(jnp.int32, (n_tok, slot_pad), 1).astype(F32)
    for i in range(per_group):
        combine[:, i * slot_pad:(i + 1) * slot_pad] = jnp.where(slot_lane == slot_cols[:, i:i + 1], 1.0, 0.0).astype(BF16)

    for k in range(N_SUB):
        drain(yrecv.at[k, pl.ds(n_exp, per_group - n_exp), pl.ds(0, cap)], y_recv.at[k])
        vals = yrecv[k].reshape(per_group * slot_pad, sub)
        hi = vals.astype(BF16)
        rest = vals - hi.astype(F32)
        mid = rest.astype(BF16)
        low = (rest - mid.astype(F32)).astype(BF16)
        sel = combine[...]
        both = jnp.dot(sel, jnp.concatenate([hi, mid], axis=1), preferred_element_type=F32)
        acc = both[:, 0:sub] + both[:, sub:] + jnp.dot(sel, low, preferred_element_type=F32)
        gpart[k] = acc.astype(BF16).reshape(n_grp, n_loc * tok, sub)
        for d in (4, 3, 5, 2, 6, 1, 7):
            go(remote(gpart.at[k, at_g(d)], grecv.at[k, d], g_send, g_recv.at[k], dev_g(d)))

    for k in range(N_SUB):
        total = gpart[k, g].astype(F32)
        drain(grecv.at[k, pl.ds(1, n_grp - 1)], g_recv.at[k])
        for d in range(1, n_grp):
            total += grecv[k, d].astype(F32)
        fin[k] = total.astype(BF16).reshape(n_loc, tok, sub)
        for d in far_first:
            go(remote(fin.at[k, at_y(d)], frecv.at[k, d], f_send, f_recv, dev_y(d)))
    drain(frecv.at[:, pl.ds(1, n_loc - 1)], f_recv)
    for k in range(N_SUB):
        for d in range(n_loc):
            cols = pl.ds(pl.multiple_of(at_y(-d) * quarter + k * sub, sub), sub)
            out_ref[:, cols] = frecv[k, d] if d else fin[k, l]
    drain(ysend.at[0, 0, 0, pl.ds(0, 8 * (2 * n_loc + 2))], m_send)
    drain(xall.at[pl.ds(0, 3), 0, pl.ds(0, 4), :, half(0)], a_send)
    drain(xall.at[pl.ds(0, 3), :, pl.ds(0, 3), :, half(0)], b_send)
    drain(xall.at[:, 0], s_send)
    drain(ysend.at[:, :, :, pl.ds(0, cap)], y_send)
    drain(grecv.at[:, pl.ds(1, n_grp - 1)], g_send)
    drain(frecv.at[:, pl.ds(1, n_loc - 1)], f_send)


def solution(mesh):
    n_grp, n_loc = mesh.shape["grp"], mesh.shape["loc"]
    tok_spec = P(("part", "grp", "loc"), None)
    w_spec = P(("grp", "loc"), None, None)

    def device_step(x_tok, expert_ids, gate_val, w_gate, w_up, w_down):
        tok, d_model = x_tok.shape
        top_k = expert_ids.shape[1]
        n_exp, _, d_ff = w_gate.shape
        n_tok = tok * n_grp * n_loc
        per_group = n_exp * n_loc
        cap = 8 * (n_tok * top_k // (4 * per_group * n_grp) + 1)
        slot_pad = -(-cap // 128) * 128
        cap_pad = -(-cap // 16) * 16
        quarter = d_model // n_loc
        sub = quarter // N_SUB
        dma = pltpu.SemaphoreType.DMA
        vmem = pl.BlockSpec(memory_space=pltpu.VMEM)
        hbm = pl.BlockSpec(memory_space=pl.ANY)
        return pl.pallas_call(
            functools.partial(layer_kernel, n_loc, n_grp, cap, top_k),
            out_shape=jax.ShapeDtypeStruct((tok, d_model), BF16),
            in_specs=[vmem, vmem, vmem, hbm, hbm, hbm],
            out_specs=vmem,
            scratch_shapes=[
                pltpu.VMEM((n_exp, d_model, d_ff), BF16),
                pltpu.VMEM((n_exp, d_model, d_ff), BF16),
                pltpu.VMEM((n_exp, n_loc, d_ff, quarter), BF16),
                pltpu.VMEM((n_grp // 2, 2, n_loc, tok, d_model), BF16),
                pltpu.VMEM((8, 128), F32),
                pltpu.VMEM((n_loc, 8, 128), F32),
                pltpu.VMEM((8, 128), F32),
                pltpu.VMEM((n_grp // 2, 2, 8, 128), F32),
                pltpu.VMEM((n_tok, n_tok), BF16),
                pltpu.VMEM((n_exp * cap_pad, n_tok), BF16),
                pltpu.VMEM((n_exp, cap_pad, d_model), BF16),
                pltpu.VMEM((n_exp, cap_pad, d_ff), F32),
                pltpu.VMEM((n_exp, cap_pad, d_ff), F32),
                pltpu.VMEM((n_exp, cap_pad, d_ff), BF16),
                pltpu.VMEM((n_tok, per_group * slot_pad), BF16),
                pltpu.VMEM((n_loc - 1, n_exp, N_SUB, cap_pad, sub), F32),
                pltpu.VMEM((N_SUB, per_group, slot_pad, sub), F32),
                pltpu.VMEM((N_SUB, n_grp, n_loc * tok, sub), BF16),
                pltpu.VMEM((N_SUB, n_grp, n_loc * tok, sub), BF16),
                pltpu.VMEM((N_SUB, n_loc, tok, sub), BF16),
                pltpu.VMEM((N_SUB, n_loc, tok, sub), BF16),
                dma((n_exp, 3)),
                dma, dma((3,)),
                dma, dma((2, 2, 3)),
                dma, dma((2, 3)),
                dma, dma((2,)),
                dma, dma((N_SUB,)),
                dma, dma((N_SUB,)),
                dma, dma,
            ],
            compiler_params=pltpu.CompilerParams(collective_id=0, has_side_effects=True, vmem_limit_bytes=64000 * 1024),
        )(x_tok, expert_ids.T, gate_val.T, w_gate, w_up, w_down)

    return jax.shard_map(device_step, mesh=mesh, in_specs=(tok_spec, tok_spec, tok_spec, w_spec, w_spec, w_spec), out_specs=tok_spec, check_vma=False)
```

```python
import functools

import jax
import jax.numpy as jnp
from jax import lax
from jax.experimental import pallas as pl
from jax.experimental.pallas import tpu as pltpu
from jax.sharding import PartitionSpec as P

MESH = pl.DeviceIdType.MESH
F32, BF16 = jnp.float32, jnp.bfloat16
N_SUB = 4
N_CHUNK = 4


def remote(src, dst, send_sem, recv_sem, device):
    return pltpu.make_async_remote_copy(src_ref=src, dst_ref=dst, send_sem=send_sem, recv_sem=recv_sem, device_id=device, device_id_type=MESH)


def drain(ref, sem):
    pltpu.make_async_copy(ref, ref, sem).wait()


def layer_kernel(n_loc, n_grp, cap, top_k, x_hbm, ids_hbm, gate_hbm, wg_hbm, wu_hbm, wd_hbm, out_ref,
                 x_ref, ids_ref, gate_ref, wg, wu, wd, xall, mown, mcol, mrow, mall, tri, picks, xg, uacc, vacc, hid, combine, ysend, yrecv, gpart, grecv, fin, frecv,
                 i_sem, w_sem, m_send, m_recv, a_send, a_recv, b_send, b_recv, s_send, s_recv,
                 y_send, y_recv, g_send, g_recv, f_send, f_recv):
    n_x = n_grp // 2
    tok, d_model = x_ref.shape
    width = d_model // N_CHUNK
    n_exp, _, d_ff = wg.shape
    per_group = n_exp * n_loc
    quarter = d_model // n_loc
    sub = quarter // N_SUB
    n_tok = n_grp * n_loc * tok
    slot_pad = yrecv.shape[2]
    cap_pad = hid.shape[1]

    l, g = lax.axis_index("loc"), lax.axis_index("grp")
    gx, gc = g // 2, g % 2

    def at_y(d):
        return (l + d + n_loc) % n_loc

    def at_x(d):
        return (gx + d + n_x) % n_x

    def at_g(d):
        return (g + d + n_grp) % n_grp

    def dev_y(d):
        return {"loc": at_y(d), "grp": g}

    def dev_x(d):
        return {"loc": l, "grp": at_x(d) * 2 + gc}

    def dev_g(d):
        return {"loc": l, "grp": at_g(d)}

    sibling = {"loc": l, "grp": gx * 2 + 1 - gc}

    barrier = pltpu.get_barrier_semaphore()
    for d in range(1, n_loc):
        pl.semaphore_signal(barrier, inc=1, device_id=dev_y(d), device_id_type=MESH)
    for d in range(1, n_grp):
        pl.semaphore_signal(barrier, inc=1, device_id=dev_g(d), device_id_type=MESH)

    inputs = [pltpu.make_async_copy(src, dst, i_sem.at[i]) for i, (src, dst) in enumerate(((ids_hbm, ids_ref), (gate_hbm, gate_ref), (x_hbm, x_ref)))]
    for c in inputs:
        c.start()

    tri_r = lax.broadcasted_iota(jnp.int32, (n_tok, n_tok), 0)
    tri_c = lax.broadcasted_iota(jnp.int32, (n_tok, n_tok), 1)
    tri[...] = jnp.where(tri_r < tri_c, 1.0, 0.0).astype(BF16)
    yrecv[:, :, cap:, :] = jnp.zeros((N_SUB, per_group, slot_pad - cap, sub), F32)
    for c in inputs:
        c.wait()
    loads = {}
    for e in range(n_exp):
        for j, (src, dst) in enumerate(((wg_hbm, wg), (wu_hbm, wu))):
            loads[e, j] = pltpu.make_async_copy(src.at[e], dst.at[e], w_sem.at[e, j])
            loads[e, j].start()
    for e in range(n_exp):
        for d in (2, 1, 3, 0):
            cols = pl.ds(pl.multiple_of(at_y(d) * quarter, quarter), quarter)
            loads[e, 2 + d] = pltpu.make_async_copy(wd_hbm.at[e, :, cols], wd.at[e, d], w_sem.at[e, 2])
            loads[e, 2 + d].start()

    lanes = n_loc * tok
    mown[...] = jnp.zeros(mown.shape, F32)
    mown[0:top_k, 0:tok] = ids_ref[...].astype(F32)
    mown[0:top_k, lanes:lanes + tok] = gate_ref[...]
    mown[...] = pltpu.roll(mown[...], l * tok, 1)
    xall[gx, gc, l] = x_ref[...]

    pl.semaphore_wait(barrier, n_loc + n_grp - 2)

    def go(copy):
        copy.start()

    far_first, near_first = (2, 1, 3), (1, 3, 2)
    for d in far_first:
        go(remote(mown, mcol.at[d], m_send, m_recv.at[0], dev_y(d)))

    def half(p):
        return pl.ds(p * 2 * width, 2 * width)

    for p in range(2):
        for d in far_first:
            for axis in range(2):
                go(remote(x_ref.at[:, half(p)], xall.at[gx, gc, l, :, half(p)], a_send, a_recv.at[axis, p, d - 1], dev_x(d) if axis else dev_y(d)))
    drain(mcol.at[pl.ds(1, n_loc - 1)], m_recv.at[0])
    mrow[...] = mown[...] + mcol[1] + mcol[2] + mcol[3]
    mall[gx, gc] = mrow[...]
    for d in far_first:
        go(remote(mrow, mall.at[gx, gc], m_send, m_recv.at[1], dev_x(d)))
    go(remote(mrow, mall.at[gx, gc], m_send, m_recv.at[2], sibling))

    def relay(p, d):
        part = xall.at[at_x(-d), gc, :, :, half(p)]
        go(remote(part, part, s_send, s_recv.at[p], sibling))

    for p in range(2):
        for d in near_first:
            for axis in range(2):
                drain(xall.at[at_x(-d), gc, l, :, half(p)] if axis else xall.at[gx, gc, at_y(-d), :, half(p)], a_recv.at[axis, p, d - 1])
                cols = pl.ds((2 * p + axis) * width, width)
                part = xall.at[at_x(-d), gc, l, :, cols] if axis else xall.at[gx, gc, at_y(-d), :, cols]
                for t in far_first:
                    go(remote(part, part, b_send, b_recv.at[p, (d if axis else t) - 1], dev_y(t) if axis else dev_x(t)))
        relay(p, 0)
        if p == 0:
            drain(mall.at[pl.ds(0, n_x - 1), 0], m_recv.at[1])
            for d in near_first:
                part = mall.at[at_x(-d), gc]
                go(remote(part, part, m_send, m_recv.at[2], sibling))

    drain(mall.at[:, 0], m_recv.at[2])
    lane = lax.broadcasted_iota(jnp.int32, mall.shape[2:], 1)
    ids = jnp.concatenate([jnp.where(lane < lanes, mall[i, 0], pltpu.roll(mall[i, 1], lanes, 1)) for i in range(n_x)], axis=1)
    gate_of = jnp.concatenate([jnp.where(lane < lanes, pltpu.roll(mall[i, 0], lanes, 1), mall[i, 1]) for i in range(n_x)], axis=1)
    row = lax.broadcasted_iota(jnp.int32, (per_group, n_tok), 0)
    row_exp = (g * per_group + ((l + n_loc - row // n_exp) % n_loc) * n_exp + row % n_exp).astype(F32)
    member = jnp.zeros(row.shape, F32)
    gates = jnp.zeros(row.shape, F32)
    for j in range(top_k):
        same = ids[j:j + 1, :] == row_exp
        member = jnp.where(same, 1.0, member)
        gates = jnp.where(same, gate_of[j:j + 1, :], gates)
    before = jnp.dot(member.astype(BF16), tri[...], preferred_element_type=F32)
    slot = jnp.where(member > 0.0, before, -1.0)
    cap_row = lax.broadcasted_iota(jnp.int32, (cap_pad, n_tok), 0).astype(F32)
    slot_gate = []
    for e in range(n_exp):
        hit = cap_row == slot[e:e + 1, :]
        picks[e * cap_pad:(e + 1) * cap_pad, :] = jnp.where(hit, 1.0, 0.0).astype(BF16)
        slot_gate.append(jnp.sum(jnp.where(hit, gates[e:e + 1, :], 0.0), axis=1, keepdims=True))

    tile = min(256, d_ff)
    tiles = [(c0, min(d_ff, c0 + tile)) for c0 in range(0, d_ff, tile)]
    for p in range(2):
        for d in near_first:
            drain(xall.at[at_x(-d), gc, pl.ds(0, n_loc - 1), :, half(p)], b_recv.at[p, d - 1])
            relay(p, d)
        drain(xall.at[:, 1 - gc, :, :, half(p)], s_recv.at[p])
        for h in (2 * p, 2 * p + 1):
            rows = xall[:, :, :, :, h * width:(h + 1) * width].reshape(n_tok, width)
            got = jnp.dot(picks[...], rows, preferred_element_type=F32).astype(BF16)
            for e in range(n_exp):
                xg[e, :, h * width:(h + 1) * width] = got[e * cap_pad:(e + 1) * cap_pad]
        k0, k1 = 2 * p * width, 2 * (p + 1) * width
        if p == 0:
            for e in range(1):
                loads[e, 0].wait()
                loads[e, 1].wait()
                for c0, c1 in tiles:
                    uacc[:, c0:c1] = jnp.dot(xg[e, :, k0:k1], wg[e, k0:k1, c0:c1], preferred_element_type=F32)
                    vacc[:, c0:c1] = jnp.dot(xg[e, :, k0:k1], wu[e, k0:k1, c0:c1], preferred_element_type=F32)
    for e in range(n_exp):
        if e:
            loads[e, 0].wait()
            loads[e, 1].wait()
        for c0, c1 in tiles:
            if e:
                u = jnp.dot(xg[e], wg[e, :, c0:c1], preferred_element_type=F32)
                v = jnp.dot(xg[e], wu[e, :, c0:c1], preferred_element_type=F32)
            else:
                u = uacc[:, c0:c1] + jnp.dot(xg[e, :, k0:k1], wg[e, k0:k1, c0:c1], preferred_element_type=F32)
                v = vacc[:, c0:c1] + jnp.dot(xg[e, :, k0:k1], wu[e, k0:k1, c0:c1], preferred_element_type=F32)
            hid[e, :, c0:c1] = (jax.nn.silu(u) * v).astype(BF16)

        def send_rows(e, k, d):
            go(remote(ysend.at[d - 1, e, k, pl.ds(0, cap)], yrecv.at[k, n_exp * d + e, pl.ds(0, cap)], y_send, y_recv.at[k], dev_y(d)))

        drain(wd.at[e], w_sem.at[e, 2])
        for d in far_first:
            o = jnp.dot(hid[e], wd[e, d], preferred_element_type=F32) * slot_gate[e]
            for k in range(N_SUB):
                ysend[d - 1, e, k] = o[:, k * sub:(k + 1) * sub]
            if e + 1 < n_exp:
                for k in range(N_SUB):
                    send_rows(e, k, d)
        if e + 1 == n_exp:
            for k in range(N_SUB):
                for d in far_first:
                    send_rows(e, k, d)
    for e in range(n_exp):
        o = jnp.dot(hid[e], wd[e, 0], preferred_element_type=F32) * slot_gate[e]
        for k in range(N_SUB):
            yrecv[k, e, 0:cap, :] = o[0:cap, k * sub:(k + 1) * sub]
    slot_cols = jnp.transpose(jnp.concatenate([slot, jnp.zeros((128 - per_group, n_tok), F32)], axis=0))
    slot_lane = lax.broadcasted_iota(jnp.int32, (n_tok, slot_pad), 1).astype(F32)
    for i in range(per_group):
        combine[:, i * slot_pad:(i + 1) * slot_pad] = jnp.where(slot_lane == slot_cols[:, i:i + 1], 1.0, 0.0).astype(BF16)

    for k in range(N_SUB):
        drain(yrecv.at[k, pl.ds(n_exp, per_group - n_exp), pl.ds(0, cap)], y_recv.at[k])
        vals = yrecv[k].reshape(per_group * slot_pad, sub)
        hi = vals.astype(BF16)
        rest = vals - hi.astype(F32)
        mid = rest.astype(BF16)
        low = (rest - mid.astype(F32)).astype(BF16)
        sel = combine[...]
        both = jnp.dot(sel, jnp.concatenate([hi, mid], axis=1), preferred_element_type=F32)
        acc = both[:, 0:sub] + both[:, sub:] + jnp.dot(sel, low, preferred_element_type=F32)
        gpart[k] = acc.astype(BF16).reshape(n_grp, n_loc * tok, sub)
        for d in (4, 3, 5, 2, 6, 1, 7):
            go(remote(gpart.at[k, at_g(d)], grecv.at[k, d], g_send, g_recv.at[k], dev_g(d)))

    for k in range(N_SUB):
        total = gpart[k, g].astype(F32)
        drain(grecv.at[k, pl.ds(1, n_grp - 1)], g_recv.at[k])
        for d in range(1, n_grp):
            total += grecv[k, d].astype(F32)
        fin[k] = total.astype(BF16).reshape(n_loc, tok, sub)
        for d in far_first:
            go(remote(fin.at[k, at_y(d)], frecv.at[k, d], f_send, f_recv, dev_y(d)))
    drain(frecv.at[:, pl.ds(1, n_loc - 1)], f_recv)
    for k in range(N_SUB):
        for d in range(n_loc):
            cols = pl.ds(pl.multiple_of(at_y(-d) * quarter + k * sub, sub), sub)
            out_ref[:, cols] = frecv[k, d] if d else fin[k, l]
    drain(ysend.at[0, 0, 0, pl.ds(0, 8 * (2 * n_loc + 2))], m_send)
    drain(xall.at[pl.ds(0, 3), 0, pl.ds(0, 4), :, half(0)], a_send)
    drain(xall.at[pl.ds(0, 3), :, pl.ds(0, 3), :, half(0)], b_send)
    drain(xall.at[:, 0], s_send)
    drain(ysend.at[:, :, :, pl.ds(0, cap)], y_send)
    drain(grecv.at[:, pl.ds(1, n_grp - 1)], g_send)
    drain(frecv.at[:, pl.ds(1, n_loc - 1)], f_send)


def solution(mesh):
    n_grp, n_loc = mesh.shape["grp"], mesh.shape["loc"]
    tok_spec = P(("part", "grp", "loc"), None)
    w_spec = P(("grp", "loc"), None, None)

    def device_step(x_tok, expert_ids, gate_val, w_gate, w_up, w_down):
        tok, d_model = x_tok.shape
        top_k = expert_ids.shape[1]
        n_exp, _, d_ff = w_gate.shape
        n_tok = tok * n_grp * n_loc
        per_group = n_exp * n_loc
        cap = 8 * (n_tok * top_k // (4 * per_group * n_grp) + 1)
        slot_pad = -(-cap // 128) * 128
        cap_pad = -(-cap // 16) * 16
        quarter = d_model // n_loc
        sub = quarter // N_SUB
        dma = pltpu.SemaphoreType.DMA
        vmem = pl.BlockSpec(memory_space=pltpu.VMEM)
        hbm = pl.BlockSpec(memory_space=pl.ANY)
        return pl.pallas_call(
            functools.partial(layer_kernel, n_loc, n_grp, cap, top_k),
            out_shape=jax.ShapeDtypeStruct((tok, d_model), BF16),
            in_specs=[hbm] * 6,
            out_specs=vmem,
            scratch_shapes=[
                pltpu.VMEM((tok, d_model), BF16),
                pltpu.VMEM((top_k, tok), jnp.int32),
                pltpu.VMEM((top_k, tok), F32),
                pltpu.VMEM((n_exp, d_model, d_ff), BF16),
                pltpu.VMEM((n_exp, d_model, d_ff), BF16),
                pltpu.VMEM((n_exp, n_loc, d_ff, quarter), BF16),
                pltpu.VMEM((n_grp // 2, 2, n_loc, tok, d_model), BF16),
                pltpu.VMEM((8, 128), F32),
                pltpu.VMEM((n_loc, 8, 128), F32),
                pltpu.VMEM((8, 128), F32),
                pltpu.VMEM((n_grp // 2, 2, 8, 128), F32),
                pltpu.VMEM((n_tok, n_tok), BF16),
                pltpu.VMEM((n_exp * cap_pad, n_tok), BF16),
                pltpu.VMEM((n_exp, cap_pad, d_model), BF16),
                pltpu.VMEM((cap_pad, d_ff), F32),
                pltpu.VMEM((cap_pad, d_ff), F32),
                pltpu.VMEM((n_exp, cap_pad, d_ff), BF16),
                pltpu.VMEM((n_tok, per_group * slot_pad), BF16),
                pltpu.VMEM((n_loc - 1, n_exp, N_SUB, cap_pad, sub), F32),
                pltpu.VMEM((N_SUB, per_group, slot_pad, sub), F32),
                pltpu.VMEM((N_SUB, n_grp, n_loc * tok, sub), BF16),
                pltpu.VMEM((N_SUB, n_grp, n_loc * tok, sub), BF16),
                pltpu.VMEM((N_SUB, n_loc, tok, sub), BF16),
                pltpu.VMEM((N_SUB, n_loc, tok, sub), BF16),
                dma((3,)),
                dma((n_exp, 3)),
                dma, dma((3,)),
                dma, dma((2, 2, 3)),
                dma, dma((2, 3)),
                dma, dma((2,)),
                dma, dma((N_SUB,)),
                dma, dma((N_SUB,)),
                dma, dma,
            ],
            compiler_params=pltpu.CompilerParams(collective_id=0, has_side_effects=True, vmem_limit_bytes=64000 * 1024),
        )(x_tok, expert_ids.T, gate_val.T, w_gate, w_up, w_down)

    return jax.shard_map(device_step, mesh=mesh, in_specs=(tok_spec, tok_spec, tok_spec, w_spec, w_spec, w_spec), out_specs=tok_spec, check_vma=False)
```

```python
import functools

import jax
import jax.numpy as jnp
from jax import lax
from jax.experimental import pallas as pl
from jax.experimental.pallas import tpu as pltpu
from jax.sharding import PartitionSpec as P

MESH = pl.DeviceIdType.MESH
F32, BF16 = jnp.float32, jnp.bfloat16
N_SUB = 4
N_CHUNK = 4


def remote(src, dst, send_sem, recv_sem, device):
    return pltpu.make_async_remote_copy(src_ref=src, dst_ref=dst, send_sem=send_sem, recv_sem=recv_sem, device_id=device, device_id_type=MESH)


def drain(ref, sem):
    pltpu.make_async_copy(ref, ref, sem).wait()


def layer_kernel(n_loc, n_grp, cap, top_k, x_hbm, ids_hbm, gate_hbm, wg_hbm, wu_hbm, wd_hbm, out_ref,
                 x_ref, ids_ref, gate_ref, wg, wu, wd, xall, mown, mcol, mrow, mall, tri, picks, xg, uacc, vacc, hid, combine, partial, ysend, yrecv, gpart, grecv, fin, frecv,
                 i_sem, w_sem, m_send, m_recv, a_send, a_recv, b_send, b_recv, s_send, s_recv,
                 y_send, y_recv, g_send, g_recv, f_send, f_recv):
    n_x = n_grp // 2
    tok, d_model = x_ref.shape
    width = d_model // N_CHUNK
    n_exp, _, d_ff = wg.shape
    per_group = n_exp * n_loc
    quarter = d_model // n_loc
    sub = quarter // N_SUB
    n_tok = n_grp * n_loc * tok
    slot_pad = yrecv.shape[2]
    cap_pad = hid.shape[1]

    l, g = lax.axis_index("loc"), lax.axis_index("grp")
    gx, gc = g // 2, g % 2

    def at_y(d):
        return (l + d + n_loc) % n_loc

    def at_x(d):
        return (gx + d + n_x) % n_x

    def at_g(d):
        return (g + d + n_grp) % n_grp

    def dev_y(d):
        return {"loc": at_y(d), "grp": g}

    def dev_x(d):
        return {"loc": l, "grp": at_x(d) * 2 + gc}

    def dev_g(d):
        return {"loc": l, "grp": at_g(d)}

    sibling = {"loc": l, "grp": gx * 2 + 1 - gc}

    barrier = pltpu.get_barrier_semaphore()
    for d in range(1, n_loc):
        pl.semaphore_signal(barrier, inc=1, device_id=dev_y(d), device_id_type=MESH)
    for d in range(1, n_grp):
        pl.semaphore_signal(barrier, inc=1, device_id=dev_g(d), device_id_type=MESH)

    inputs = [pltpu.make_async_copy(src, dst, i_sem.at[i]) for i, (src, dst) in enumerate(((ids_hbm, ids_ref), (gate_hbm, gate_ref), (x_hbm, x_ref)))]
    for c in inputs:
        c.start()

    tri_r = lax.broadcasted_iota(jnp.int32, (n_tok, n_tok), 0)
    tri_c = lax.broadcasted_iota(jnp.int32, (n_tok, n_tok), 1)
    tri[...] = jnp.where(tri_r < tri_c, 1.0, 0.0).astype(BF16)
    yrecv[:, :, cap:, :] = jnp.zeros((N_SUB, per_group, slot_pad - cap, sub), F32)
    for c in inputs:
        c.wait()
    loads = {}
    for e in range(n_exp):
        for j, (src, dst) in enumerate(((wg_hbm, wg), (wu_hbm, wu))):
            loads[e, j] = pltpu.make_async_copy(src.at[e], dst.at[e], w_sem.at[e, j])
            loads[e, j].start()
    for e in range(n_exp):
        for d in (2, 1, 3, 0):
            cols = pl.ds(pl.multiple_of(at_y(d) * quarter, quarter), quarter)
            loads[e, 2 + d] = pltpu.make_async_copy(wd_hbm.at[e, :, cols], wd.at[e, d], w_sem.at[e, 2])
            loads[e, 2 + d].start()

    lanes = n_loc * tok
    mown[...] = jnp.zeros(mown.shape, F32)
    mown[0:top_k, 0:tok] = ids_ref[...].astype(F32)
    mown[0:top_k, lanes:lanes + tok] = gate_ref[...]
    mown[...] = pltpu.roll(mown[...], l * tok, 1)
    xall[gx, gc, l] = x_ref[...]

    pl.semaphore_wait(barrier, n_loc + n_grp - 2)

    def go(copy):
        copy.start()

    far_first, near_first = (2, 1, 3), (1, 3, 2)
    for d in far_first:
        go(remote(mown, mcol.at[d], m_send, m_recv.at[0], dev_y(d)))

    def half(p):
        return pl.ds(p * 2 * width, 2 * width)

    for p in range(2):
        for d in far_first:
            for axis in range(2):
                go(remote(x_ref.at[:, half(p)], xall.at[gx, gc, l, :, half(p)], a_send, a_recv.at[axis, p, d - 1], dev_x(d) if axis else dev_y(d)))
    drain(mcol.at[pl.ds(1, n_loc - 1)], m_recv.at[0])
    mrow[...] = mown[...] + mcol[1] + mcol[2] + mcol[3]
    mall[gx, gc] = mrow[...]
    for d in far_first:
        go(remote(mrow, mall.at[gx, gc], m_send, m_recv.at[1], dev_x(d)))
    go(remote(mrow, mall.at[gx, gc], m_send, m_recv.at[2], sibling))

    def relay(p, d):
        part = xall.at[at_x(-d), gc, :, :, half(p)]
        go(remote(part, part, s_send, s_recv.at[p], sibling))

    for p in range(2):
        for d in near_first:
            for axis in range(2):
                drain(xall.at[at_x(-d), gc, l, :, half(p)] if axis else xall.at[gx, gc, at_y(-d), :, half(p)], a_recv.at[axis, p, d - 1])
                cols = pl.ds((2 * p + axis) * width, width)
                part = xall.at[at_x(-d), gc, l, :, cols] if axis else xall.at[gx, gc, at_y(-d), :, cols]
                for t in far_first:
                    go(remote(part, part, b_send, b_recv.at[p, (d if axis else t) - 1], dev_y(t) if axis else dev_x(t)))
        relay(p, 0)
        if p == 0:
            drain(mall.at[pl.ds(0, n_x - 1), 0], m_recv.at[1])
            for d in near_first:
                part = mall.at[at_x(-d), gc]
                go(remote(part, part, m_send, m_recv.at[2], sibling))

    drain(mall.at[:, 0], m_recv.at[2])
    lane = lax.broadcasted_iota(jnp.int32, mall.shape[2:], 1)
    ids = jnp.concatenate([jnp.where(lane < lanes, mall[i, 0], pltpu.roll(mall[i, 1], lanes, 1)) for i in range(n_x)], axis=1)
    gate_of = jnp.concatenate([jnp.where(lane < lanes, pltpu.roll(mall[i, 0], lanes, 1), mall[i, 1]) for i in range(n_x)], axis=1)
    row = lax.broadcasted_iota(jnp.int32, (per_group, n_tok), 0)
    row_exp = (g * per_group + ((l + n_loc - row % n_loc) % n_loc) * n_exp + row // n_loc).astype(F32)
    member = jnp.zeros(row.shape, F32)
    gates = jnp.zeros(row.shape, F32)
    for j in range(top_k):
        same = ids[j:j + 1, :] == row_exp
        member = jnp.where(same, 1.0, member)
        gates = jnp.where(same, gate_of[j:j + 1, :], gates)
    before = jnp.dot(member.astype(BF16), tri[...], preferred_element_type=F32)
    slot = jnp.where(member > 0.0, before, -1.0)
    cap_row = lax.broadcasted_iota(jnp.int32, (cap_pad, n_tok), 0).astype(F32)
    slot_gate = []
    for e in range(n_exp):
        hit = cap_row == slot[e * n_loc:e * n_loc + 1, :]
        picks[e * cap_pad:(e + 1) * cap_pad, :] = jnp.where(hit, 1.0, 0.0).astype(BF16)
        slot_gate.append(jnp.sum(jnp.where(hit, gates[e * n_loc:e * n_loc + 1, :], 0.0), axis=1, keepdims=True))

    tile = min(256, d_ff)
    tiles = [(c0, min(d_ff, c0 + tile)) for c0 in range(0, d_ff, tile)]
    for p in range(2):
        for d in near_first:
            drain(xall.at[at_x(-d), gc, pl.ds(0, n_loc - 1), :, half(p)], b_recv.at[p, d - 1])
            relay(p, d)
        drain(xall.at[:, 1 - gc, :, :, half(p)], s_recv.at[p])
        for h in (2 * p, 2 * p + 1):
            rows = xall[:, :, :, :, h * width:(h + 1) * width].reshape(n_tok, width)
            got = jnp.dot(picks[...], rows, preferred_element_type=F32).astype(BF16)
            for e in range(n_exp):
                xg[e, :, h * width:(h + 1) * width] = got[e * cap_pad:(e + 1) * cap_pad]
        k0, k1 = 2 * p * width, 2 * (p + 1) * width
        if p == 0:
            for e in range(1):
                loads[e, 0].wait()
                loads[e, 1].wait()
                for c0, c1 in tiles:
                    uacc[:, c0:c1] = jnp.dot(xg[e, :, k0:k1], wg[e, k0:k1, c0:c1], preferred_element_type=F32)
                    vacc[:, c0:c1] = jnp.dot(xg[e, :, k0:k1], wu[e, k0:k1, c0:c1], preferred_element_type=F32)
    for e in range(n_exp):
        if e:
            loads[e, 0].wait()
            loads[e, 1].wait()
        for c0, c1 in tiles:
            if e:
                u = jnp.dot(xg[e], wg[e, :, c0:c1], preferred_element_type=F32)
                v = jnp.dot(xg[e], wu[e, :, c0:c1], preferred_element_type=F32)
            else:
                u = uacc[:, c0:c1] + jnp.dot(xg[e, :, k0:k1], wg[e, k0:k1, c0:c1], preferred_element_type=F32)
                v = vacc[:, c0:c1] + jnp.dot(xg[e, :, k0:k1], wu[e, k0:k1, c0:c1], preferred_element_type=F32)
            hid[e, :, c0:c1] = (jax.nn.silu(u) * v).astype(BF16)

        def send_rows(e, k, d):
            go(remote(ysend.at[d - 1, e, k, pl.ds(0, cap)], yrecv.at[k, n_loc * e + d, pl.ds(0, cap)], y_send, y_recv.at[e, k], dev_y(d)))

        drain(wd.at[e], w_sem.at[e, 2])
        for d in far_first:
            o = jnp.dot(hid[e], wd[e, d], preferred_element_type=F32) * slot_gate[e]
            for k in range(N_SUB):
                ysend[d - 1, e, k] = o[:, k * sub:(k + 1) * sub]
            if e + 1 < n_exp:
                for k in range(N_SUB):
                    send_rows(e, k, d)
        if e + 1 == n_exp:
            for k in range(N_SUB):
                for d in far_first:
                    send_rows(e, k, d)
    for e in range(n_exp):
        o = jnp.dot(hid[e], wd[e, 0], preferred_element_type=F32) * slot_gate[e]
        for k in range(N_SUB):
            yrecv[k, n_loc * e, 0:cap, :] = o[0:cap, k * sub:(k + 1) * sub]
    slot_cols = jnp.transpose(jnp.concatenate([slot, jnp.zeros((128 - per_group, n_tok), F32)], axis=0))
    slot_lane = lax.broadcasted_iota(jnp.int32, (n_tok, slot_pad), 1).astype(F32)
    for i in range(per_group):
        combine[:, i * slot_pad:(i + 1) * slot_pad] = jnp.where(slot_lane == slot_cols[:, i:i + 1], 1.0, 0.0).astype(BF16)

    def token_sums(e, k):
        drain(yrecv.at[k, pl.ds(n_loc * e + 1, n_loc - 1), pl.ds(0, cap)], y_recv.at[e, k])
        vals = yrecv[k, n_loc * e:n_loc * (e + 1)].reshape(n_loc * slot_pad, sub)
        hi = vals.astype(BF16)
        rest = vals - hi.astype(F32)
        mid = rest.astype(BF16)
        low = (rest - mid.astype(F32)).astype(BF16)
        sel = combine[:, e * n_loc * slot_pad:(e + 1) * n_loc * slot_pad]
        both = jnp.dot(sel, jnp.concatenate([hi, mid], axis=1), preferred_element_type=F32)
        return both[:, 0:sub] + both[:, sub:] + jnp.dot(sel, low, preferred_element_type=F32)

    for k in range(N_SUB):
        partial[k] = token_sums(0, k)
    for k in range(N_SUB):
        acc = partial[k]
        for e in range(1, n_exp):
            acc += token_sums(e, k)
        gpart[k] = acc.astype(BF16).reshape(n_grp, n_loc * tok, sub)
        for d in (4, 3, 5, 2, 6, 1, 7):
            go(remote(gpart.at[k, at_g(d)], grecv.at[k, d], g_send, g_recv.at[k], dev_g(d)))

    for k in range(N_SUB):
        total = gpart[k, g].astype(F32)
        drain(grecv.at[k, pl.ds(1, n_grp - 1)], g_recv.at[k])
        for d in range(1, n_grp):
            total += grecv[k, d].astype(F32)
        fin[k] = total.astype(BF16).reshape(n_loc, tok, sub)
        for d in far_first:
            go(remote(fin.at[k, at_y(d)], frecv.at[k, d], f_send, f_recv, dev_y(d)))
    drain(frecv.at[:, pl.ds(1, n_loc - 1)], f_recv)
    for k in range(N_SUB):
        for d in range(n_loc):
            cols = pl.ds(pl.multiple_of(at_y(-d) * quarter + k * sub, sub), sub)
            out_ref[:, cols] = frecv[k, d] if d else fin[k, l]
    drain(ysend.at[0, 0, 0, pl.ds(0, 8 * (2 * n_loc + 2))], m_send)
    drain(xall.at[pl.ds(0, 3), 0, pl.ds(0, 4), :, half(0)], a_send)
    drain(xall.at[pl.ds(0, 3), :, pl.ds(0, 3), :, half(0)], b_send)
    drain(xall.at[:, 0], s_send)
    drain(ysend.at[:, :, :, pl.ds(0, cap)], y_send)
    drain(grecv.at[:, pl.ds(1, n_grp - 1)], g_send)
    drain(frecv.at[:, pl.ds(1, n_loc - 1)], f_send)


def solution(mesh):
    n_grp, n_loc = mesh.shape["grp"], mesh.shape["loc"]
    tok_spec = P(("part", "grp", "loc"), None)
    w_spec = P(("grp", "loc"), None, None)

    def device_step(x_tok, expert_ids, gate_val, w_gate, w_up, w_down):
        tok, d_model = x_tok.shape
        top_k = expert_ids.shape[1]
        n_exp, _, d_ff = w_gate.shape
        n_tok = tok * n_grp * n_loc
        per_group = n_exp * n_loc
        cap = 8 * (n_tok * top_k // (4 * per_group * n_grp) + 1)
        slot_pad = -(-cap // 128) * 128
        cap_pad = -(-cap // 16) * 16
        quarter = d_model // n_loc
        sub = quarter // N_SUB
        dma = pltpu.SemaphoreType.DMA
        vmem = pl.BlockSpec(memory_space=pltpu.VMEM)
        hbm = pl.BlockSpec(memory_space=pl.ANY)
        return pl.pallas_call(
            functools.partial(layer_kernel, n_loc, n_grp, cap, top_k),
            out_shape=jax.ShapeDtypeStruct((tok, d_model), BF16),
            in_specs=[hbm] * 6,
            out_specs=vmem,
            scratch_shapes=[
                pltpu.VMEM((tok, d_model), BF16),
                pltpu.VMEM((top_k, tok), jnp.int32),
                pltpu.VMEM((top_k, tok), F32),
                pltpu.VMEM((n_exp, d_model, d_ff), BF16),
                pltpu.VMEM((n_exp, d_model, d_ff), BF16),
                pltpu.VMEM((n_exp, n_loc, d_ff, quarter), BF16),
                pltpu.VMEM((n_grp // 2, 2, n_loc, tok, d_model), BF16),
                pltpu.VMEM((8, 128), F32),
                pltpu.VMEM((n_loc, 8, 128), F32),
                pltpu.VMEM((8, 128), F32),
                pltpu.VMEM((n_grp // 2, 2, 8, 128), F32),
                pltpu.VMEM((n_tok, n_tok), BF16),
                pltpu.VMEM((n_exp * cap_pad, n_tok), BF16),
                pltpu.VMEM((n_exp, cap_pad, d_model), BF16),
                pltpu.VMEM((cap_pad, d_ff), F32),
                pltpu.VMEM((cap_pad, d_ff), F32),
                pltpu.VMEM((n_exp, cap_pad, d_ff), BF16),
                pltpu.VMEM((n_tok, per_group * slot_pad), BF16),
                pltpu.VMEM((N_SUB, n_tok, sub), F32),
                pltpu.VMEM((n_loc - 1, n_exp, N_SUB, cap_pad, sub), F32),
                pltpu.VMEM((N_SUB, per_group, slot_pad, sub), F32),
                pltpu.VMEM((N_SUB, n_grp, n_loc * tok, sub), BF16),
                pltpu.VMEM((N_SUB, n_grp, n_loc * tok, sub), BF16),
                pltpu.VMEM((N_SUB, n_loc, tok, sub), BF16),
                pltpu.VMEM((N_SUB, n_loc, tok, sub), BF16),
                dma((3,)),
                dma((n_exp, 3)),
                dma, dma((3,)),
                dma, dma((2, 2, 3)),
                dma, dma((2, 3)),
                dma, dma((2,)),
                dma, dma((n_exp, N_SUB)),
                dma, dma((N_SUB,)),
                dma, dma,
            ],
            compiler_params=pltpu.CompilerParams(collective_id=0, has_side_effects=True, vmem_limit_bytes=64000 * 1024),
        )(x_tok, expert_ids.T, gate_val.T, w_gate, w_up, w_down)

    return jax.shard_map(device_step, mesh=mesh, in_specs=(tok_spec, tok_spec, tok_spec, w_spec, w_spec, w_spec), out_specs=tok_spec, check_vma=False)
```
